32 devices in a mesh: seq: 16 (over z, y, core), dp: 2 (over x).
Axes of the slice: x: 2, y: 2, z: 4, core: 2. Of those that a mesh axis runs over, the one named last changes fastest.
Arguments:
- acceptors: bfloat16 [2, 2048, 2560], P('dp', 'seq'), may hold values from -2 to 2
- lookups: bfloat16 [2, 2048, 2560], P('dp', 'seq'), may hold values from -0.625 to 0.625
- payloads: bfloat16 [2, 2048, 2560], P('dp', 'seq'), may hold values from -6 to 6
- lagged_fading_source: bfloat16 [2, 2048, 2560], P('dp', 'seq'), may hold values from -6 to 6
- response_cotangent: bfloat16 [2, 2048, 2560], P('dp', 'seq'), may hold values from -5 to 5
- fading_lowering_array: bfloat16 [2560, 128], replicated, may hold values from -0.125 to 0.125
- fading_raising_array: bfloat16 [2560, 128], replicated, may hold values from -1.25 to 1.25
- feature_fading_speed: float32 [2560], replicated, may hold values from 2.3251488e-05 to 0.125
- present_reward: float32 [2560], replicated, may hold values from 1.4142135 to 11.313708
Outputs:
- mixed: bfloat16 [2, 2048, 2560], P('dp', 'seq')
- grad_receptance: bfloat16 [2, 2048, 2560], P('dp', 'seq')
- lookup_deriv: bfloat16 [2, 2048, 2560], P('dp', 'seq')
- payload_deriv: bfloat16 [2, 2048, 2560], P('dp', 'seq')
- grad_decay_input: bfloat16 [2, 2048, 2560], P('dp', 'seq')
- grad_lora_a: float32 [2560, 128], P('dp')
- grad_lora_b: float32 [2560, 128], P('dp')
- grad_time_decay: float32 [2560], P('dp')
- present_reward_deriv: float32 [2560], P('dp')
The draws below stay inside these ranges and needn't reach their ends.
All inputs are finite; a program needn't handle non-finite values.
Results may differ from the reference program's by a relative error of at most 0.006.
Values sent between devices are 32-bit elements.
A program may use at most 320 MiB of HBM per device.

```python
import math
import jax
import jax.numpy as jnp
from jax import lax

ATTENDER_TOTAL = 40
LANE_TOTAL = 64
DECAY_RANK = 128
BLOCK = 64
EMBED_SPAN = 2560
SEQLEN = 2048
SEQS = 2


def draw_feature_fading_speed(key, part):
    choose_key, slow_key, fast_key, corner_key = jax.random.split(jax.random.fold_in(key, 7), 4)
    slower = jnp.exp(jax.random.uniform(slow_key, (EMBED_SPAN,), jnp.float32, math.log(0.05), math.log(0.6))) / SEQLEN
    faster = 1.0 / jax.random.uniform(fast_key, (EMBED_SPAN,), jnp.float32, 8.0, 40.0)
    lasting = jax.random.uniform(choose_key, (EMBED_SPAN,), jnp.float32) < 0.5
    rates = jnp.where(lasting, slower, faster)
    return jnp.clip(rates, 0.05 / SEQLEN, 0.125).astype(jnp.float32)


def block_levels(own_key, shape, cuts, low, high):
    def one(dim, parts):
        heights = jax.random.uniform(jax.random.fold_in(jax.random.fold_in(own_key, 6), dim), (parts,), jnp.float32, low / len(cuts), high / len(cuts))
        return jnp.repeat(jnp.exp(heights), shape[dim] // parts).reshape((-1,) + (1,) * (len(shape) - dim - 1))

    factor_of = one(*cuts[0])
    for cut in cuts[1:]:
        factor_of = factor_of * one(*cut)
    return factor_of


def centred(own_key, dims, spread, limit, pieces=(), dtype=jnp.bfloat16):
    array = jax.random.normal(own_key, dims, jnp.float32) * spread
    if len(pieces) > 0:
        array = block_levels(own_key, dims, pieces, -0.22, 0.18) * array
    return jnp.clip(array, min=-limit, max=limit).astype(dtype)


def setup_inputs(seed: int = 0) -> dict:
    key_list = jax.random.split(jax.random.key(seed), 10)
    acceptors = centred(key_list[0], (SEQS, SEQLEN, EMBED_SPAN), (LANE_TOTAL ** -0.5), 2.0, ((0, 2), (1, 16)))
    lookups = centred(key_list[1], (SEQS, SEQLEN, EMBED_SPAN), (2.0 / SEQLEN ** 0.5), 0.625, ((0, 2), (1, 16)))
    payloads = centred(key_list[2], (SEQS, SEQLEN, EMBED_SPAN), 1.0, 6.0, ((0, 2), (1, 16)))
    lagged_fading_source = centred(key_list[3], (SEQS, SEQLEN, EMBED_SPAN), 1.0, 6.0, ((0, 2), (1, 16)))
    response_cotangent = centred(key_list[4], (SEQS, SEQLEN, EMBED_SPAN), (16.0 / SEQLEN ** 0.5), 5.0, ((0, 2), (1, 16)))
    fading_lowering_array = centred(key_list[5], (EMBED_SPAN, DECAY_RANK), EMBED_SPAN ** -0.5, 0.125)
    fading_raising_array = centred(key_list[6], (EMBED_SPAN, DECAY_RANK), 0.08, 1.25)
    feature_fading_speed = draw_feature_fading_speed(jax.random.fold_in(key_list[9], 71), 0)
    present_reward = jnp.clip(jnp.exp(jax.random.uniform(key_list[8], (EMBED_SPAN,), jnp.float32, math.log(1.4142135), math.log(11.313708))), 1.4142135, 11.313708)
    return dict(acceptors=acceptors, lookups=lookups, payloads=payloads, lagged_fading_source=lagged_fading_source, response_cotangent=response_cotangent, fading_lowering_array=fading_lowering_array, fading_raising_array=fading_raising_array, feature_fading_speed=feature_fading_speed, present_reward=present_reward)


HIGH = lax.Precision.HIGHEST


def contract(pattern, left, right):
    return jnp.einsum(pattern, left, right, precision=HIGH, preferred_element_type=jnp.float32)


def decay_log_values(input_rows, fading_lowering_array, fading_raising_array, feature_fading_speed):
    apply_projection = jnp.dot(input_rows, fading_lowering_array, preferred_element_type=jnp.float32)
    smoothed_values = jnp.tanh(apply_projection)
    gate_portion = smoothed_values.astype(jnp.bfloat16)
    rank_projection = lax.dot_general(gate_portion, fading_raising_array, (((1,), (1,)), ((), ())), preferred_element_type=jnp.float32)
    return smoothed_values, gate_portion, -feature_fading_speed[None, :] * jnp.exp(rank_projection)


def compose(decays, own_states, backward):
    def advance(carry, member):
        run_decay, run_state = carry
        decay, own_state = member
        return (run_decay * decay, decay[..., None] * run_state + own_state), carry

    initial = (jnp.ones(decays.shape[1:], jnp.float32), jnp.zeros(own_states.shape[1:], jnp.float32))
    return lax.scan(advance, initial, (decays, own_states), reverse=backward)


def temporal_blend_sublevel(acceptor_lines, lookups, payloads, incoming_cotangent, fading_exponent, reward_by_attender, adjacent_shardlink):
    inclusive = jnp.cumsum(fading_exponent, axis=1)
    exclusive = inclusive - fading_exponent
    middle = inclusive[:, BLOCK // 2 - 1:BLOCK // 2]
    overall = inclusive[:, -1]
    entering = jnp.exp(exclusive)
    leaving = jnp.exp(overall[:, None] - inclusive)
    upward = jnp.exp(exclusive - middle)
    downward = jnp.exp(middle - inclusive)
    decays = jnp.exp(overall)
    reached = acceptor_lines * entering
    faded_keys = lookups * leaving
    own_states = contract("nchk,nchv->nhkv", faded_keys, payloads)
    pull_states = contract("nchk,nchv->nhkv", reached, incoming_cotangent)
    starts, block_ends = adjacent_shardlink(decays, own_states, pull_states)
    position = jnp.arange(BLOCK)
    beneath = position[:, None] > position[None, :]
    early_recept = acceptor_lines * upward
    late_keys = lookups * downward
    scores = jnp.where(beneath, contract("nthk,nshk->nhts", early_recept, late_keys), 0.0)
    present_contribution = jnp.sum(acceptor_lines * reward_by_attender * lookups, axis=-1)[..., None]
    blended_response = contract("nhts,nshv->nthv", scores, payloads) + present_contribution * payloads + contract("nthk,nhkv->nthv", reached, starts)
    grad_start = decays[..., None] * block_ends + pull_states
    products = jnp.where(beneath, contract("nthv,nshv->nhts", incoming_cotangent, payloads), 0.0)
    agreement_verify = jnp.sum(payloads * incoming_cotangent, axis=-1)[..., None]
    memory_acceptors = entering * contract("nhkv,nthv->nthk", starts, incoming_cotangent) + upward * contract("nhts,nshk->nthk", products, late_keys)
    memory_lookup_lines = leaving * contract("nhkv,nthv->nthk", block_ends, payloads) + downward * contract("nhst,nshk->nthk", products, early_recept)
    payload_deriv = contract("nthk,nhkv->nthv", faded_keys, block_ends) + contract("nhst,nshv->nthv", scores, incoming_cotangent) + present_contribution * incoming_cotangent
    acceptor_deriv = memory_acceptors + reward_by_attender * lookups * agreement_verify
    lookup_deriv = memory_lookup_lines + reward_by_attender * acceptor_lines * agreement_verify
    present_reward_deriv = jnp.sum(acceptor_lines * lookups * agreement_verify, axis=(0, 1))
    coupling = jnp.sum(grad_start * starts, axis=-1)
    change = lookups * memory_lookup_lines - acceptor_lines * memory_acceptors
    fading_deriv = coupling[:, None] + jnp.cumsum(change, axis=1) - change - acceptor_lines * memory_acceptors
    return blended_response, acceptor_deriv, lookup_deriv, payload_deriv, fading_deriv, present_reward_deriv


def sublevel_evaluation(reshaped_acceptors, reshaped_lookups, reshaped_payloads, reshaped_source, incoming_cotangent_reshaped, fading_lowering_array, fading_raising_array, feature_fading_speed, present_reward, adjacent_shardlink):
    smoothed_values, gate_portion, fading_exponent = decay_log_values(reshaped_source, fading_lowering_array, fading_raising_array, feature_fading_speed)
    tokens, feature_span = reshaped_acceptors.shape
    tiling_arrangement = (tokens // BLOCK, BLOCK, ATTENDER_TOTAL, LANE_TOTAL)
    collected_outcomes = temporal_blend_sublevel(reshaped_acceptors.astype(jnp.float32).reshape(tiling_arrangement),
                       reshaped_lookups.astype(jnp.float32).reshape(tiling_arrangement),
                       reshaped_payloads.astype(jnp.float32).reshape(tiling_arrangement),
                       incoming_cotangent_reshaped.astype(jnp.float32).reshape(tiling_arrangement),
                       fading_exponent.reshape(tiling_arrangement), present_reward.reshape(ATTENDER_TOTAL, LANE_TOTAL), adjacent_shardlink)
    blended_response, acceptor_deriv, lookup_deriv, payload_deriv, fading_deriv, present_reward_deriv = collected_outcomes
    slope = fading_deriv.reshape(tokens, feature_span) * fading_exponent
    slope_portion = slope.astype(jnp.bfloat16)
    gate_gradient = jnp.dot(slope_portion, fading_raising_array, preferred_element_type=jnp.float32)
    projection_gradient = (gate_gradient * (1.0 - smoothed_values * smoothed_values)).astype(jnp.bfloat16)
    input_gradient = lax.dot_general(projection_gradient, fading_lowering_array, (((1,), (1,)), ((), ())), preferred_element_type=jnp.float32).astype(jnp.bfloat16)
    lowering_array_deriv = lax.dot_general(reshaped_source, projection_gradient, (((0,), (0,)), ((), ())), preferred_element_type=jnp.float32)
    raising_array_deriv = lax.dot_general(slope_portion, gate_portion, (((0,), (0,)), ((), ())), preferred_element_type=jnp.float32)
    speed_deriv = jnp.sum(slope, axis=0)

    def flatten(member):
        return member.reshape(tokens, feature_span).astype(jnp.bfloat16)

    return (flatten(blended_response), flatten(acceptor_deriv), flatten(lookup_deriv), flatten(payload_deriv), input_gradient,
            (lowering_array_deriv, raising_array_deriv, speed_deriv, present_reward_deriv.reshape(feature_span)))


def sharded_ownlink(decays, own_states, pull_states):
    ahead_total, ahead = compose(decays, own_states, False)
    behind_total, behind = compose(decays, pull_states, True)
    return ahead[1], behind[1]


def reference(acceptors, lookups, payloads, lagged_fading_source, response_cotangent, fading_lowering_array, fading_raising_array, feature_fading_speed, present_reward):
    collected = []
    for symbol_stream in range(acceptors.shape[0]):
        collected.append(sublevel_evaluation(acceptors[symbol_stream], lookups[symbol_stream], payloads[symbol_stream], lagged_fading_source[symbol_stream],
                                    response_cotangent[symbol_stream], fading_lowering_array, fading_raising_array, feature_fading_speed, present_reward, sharded_ownlink))
    stacked = [jnp.stack([member[index] for member in collected]) for index in range(5)]
    summed = [jnp.sum(jnp.stack([member[5][index] for member in collected]), axis=0) for index in range(4)]
    return (stacked[0], stacked[1], stacked[2], stacked[3], stacked[4], summed[0], summed[1], summed[2], summed[3])
```

```python
import functools
import jax
import jax.numpy as jnp
from jax import lax
from jax.experimental import pallas as pl
from jax.experimental.pallas import tpu as pltpu
from jax.sharding import PartitionSpec as P

LANE_TOTAL = 64
BLOCK = 64
PAIR = 2 * LANE_TOTAL
F32 = jnp.float32
BF16 = jnp.bfloat16
GONE = -1e30
SKEW = 4
GRAIN = 512


def nn(a, b):
    return lax.dot_general(a, b, (((1,), (0,)), ((), ())), preferred_element_type=F32)


def nt(a, b):
    return lax.dot_general(a, b, (((1,), (1,)), ((), ())), preferred_element_type=F32)


def tn(a, b):
    return lax.dot_general(a, b, (((0,), (0,)), ((), ())), preferred_element_type=F32)


def split(a, terms):
    out = []
    for _ in range(terms):
        out.append(a.astype(BF16))
        a = a - out[-1].astype(F32)
    return out


def exact_left(m, a, terms):
    return sum(nn(m, t) for t in split(a, terms))


def exact_right(a, m, terms):
    return sum(nn(t, m) for t in split(a, terms))


def triangle(n, strict):
    row = lax.broadcasted_iota(jnp.int32, (n, n), 0)
    col = lax.broadcasted_iota(jnp.int32, (n, n), 1)
    keep = row > col if strict else row >= col
    return jnp.where(keep, 1.0, 0.0).astype(BF16)


def diagonal_heads(m):
    lane = lax.broadcasted_iota(jnp.int32, (LANE_TOTAL, PAIR), 1)
    return jnp.where(lane < LANE_TOTAL, m[:LANE_TOTAL], m[LANE_TOTAL:])


def totals_kernel(
    x_ref, a_ref, b_ref, speed_ref, r_ref, k_ref, v_ref, g_ref,
    th_ref, w_ref, incl_ref, own_ref, pull_ref, dec_ref,
):
    tokens = x_ref.shape[0]

    @pl.when(pl.program_id(0) == 0)
    def _():
        th_ref[...] = jnp.tanh(nn(x_ref[...], a_ref[...]))

    gate = th_ref[...].astype(BF16)
    w = -speed_ref[0] * jnp.exp(nt(gate, b_ref[...]))
    incl = exact_left(triangle(tokens, False), w, 3)
    total = incl[tokens - 1 :]
    w_ref[...] = w
    incl_ref[...] = incl
    faded = k_ref[...].astype(F32) * jnp.exp(total - incl)
    reached = r_ref[...].astype(F32) * jnp.exp(incl - w)
    own_ref[0] = diagonal_heads(sum(tn(v_ref[...], t) for t in split(faded, 2)))
    pull_ref[0] = diagonal_heads(sum(tn(g_ref[...], t) for t in split(reached, 2)))
    dec_ref[0] = jnp.exp(total)


def chain_kernel(own_ref, pull_ref, dec_ref, s_ref, g_ref, so_ref, go_ref, sf, rf, sb, rb):
    n = lax.axis_size("seq")
    me = lax.axis_index("seq")
    pairs = own_ref.shape[0]
    right = lax.rem(me + 1, n)
    left = lax.rem(me + n - 1, n)
    barrier = pltpu.get_barrier_semaphore()
    for neighbour in (left, right):
        pl.semaphore_signal(
            barrier, inc=1, device_id={"seq": neighbour}, device_id_type=pl.DeviceIdType.MESH
        )
    pl.semaphore_wait(barrier, 2)

    def forward(c):
        return pltpu.make_async_remote_copy(
            src_ref=so_ref.at[c], dst_ref=s_ref.at[c], send_sem=sf.at[c], recv_sem=rf.at[c],
            device_id={"seq": right}, device_id_type=pl.DeviceIdType.MESH,
        )

    def backward(c):
        return pltpu.make_async_remote_copy(
            src_ref=go_ref.at[c], dst_ref=g_ref.at[c], send_sem=sb.at[c], recv_sem=rb.at[c],
            device_id={"seq": left}, device_id_type=pl.DeviceIdType.MESH,
        )

    def relay(c, first, last, copy, in_ref, out_ref, add_ref):
        @pl.when((c >= 0) & (c < pairs))
        def _():
            @pl.when(first)
            def _():
                in_ref[c] = jnp.zeros(in_ref.shape[1:], F32)

            @pl.when(jnp.logical_not(first))
            def _():
                copy(c).wait_recv()

            @pl.when(jnp.logical_not(last))
            def _():
                out_ref[c] = dec_ref[c] * in_ref[c] + add_ref[c]
                copy(c).start()

    at_start = me == 0
    at_end = me == n - 1

    def step(s, carry):
        relay(s - SKEW * me, at_start, at_end, forward, s_ref, so_ref, own_ref)
        relay(s - SKEW * (n - 1 - me), at_end, at_start, backward, g_ref, go_ref, pull_ref)
        return carry

    lax.fori_loop(0, SKEW * (n - 1) + pairs, step, 0)

    def finish(c, carry):
        @pl.when(jnp.logical_not(at_end))
        def _():
            forward(c).wait_send()

        @pl.when(jnp.logical_not(at_start))
        def _():
            backward(c).wait_send()

        return carry

    lax.fori_loop(0, pairs, finish, 0)


def finish_kernel(
    x_ref, a_ref, b_ref, u_ref, r_ref, k_ref, v_ref, g_ref,
    th_ref, w_ref, incl_ref, pull_ref, dec_ref, s_ref, ga_ref,
    mixed_ref, dr_ref, dk_ref, dv_ref, dx_ref, sums_ref, db_ref, acc_ref,
):
    tokens, span = x_ref.shape
    pair = pl.program_id(0)
    pairs = pl.num_programs(0)

    @pl.when(pair == 0)
    def _():
        sums_ref[span:, :] = jnp.zeros((sums_ref.shape[0] - span, sums_ref.shape[1]), F32)

    row = lax.broadcasted_iota(jnp.int32, (tokens, PAIR), 0)
    lane = lax.broadcasted_iota(jnp.int32, (tokens, PAIR), 1)
    at = lax.broadcasted_iota(jnp.int32, (tokens, tokens), 0)
    of = lax.broadcasted_iota(jnp.int32, (tokens, tokens), 1)
    near = (at > of) & (at // BLOCK == of // BLOCK)
    far = (at >= BLOCK) & (of < BLOCK)
    low = lane < LANE_TOTAL
    upper = row < BLOCK
    zero = jnp.zeros((tokens, PAIR), BF16)

    def heads(a):
        return jnp.where(low, a, zero), jnp.where(low, zero, a)

    rb, kb, vb, gb = r_ref[...], k_ref[...], v_ref[...], g_ref[...]
    r, k, v, g = rb.astype(F32), kb.astype(F32), vb.astype(F32), gb.astype(F32)
    w, incl = w_ref[...], incl_ref[...]
    u = u_ref[0]
    excl = incl - w
    total = incl[tokens - 1 :]
    half = BLOCK // 2
    middle = jnp.where(upper, incl[half - 1 : half], incl[BLOCK + half - 1 : BLOCK + half])
    edge = incl[BLOCK - 1 : BLOCK]
    upward = jnp.exp(excl - middle)
    downward = jnp.exp(middle - incl)
    entering = jnp.exp(excl)
    leaving = jnp.exp(total - incl)
    past_edge = jnp.exp(jnp.where(upper, GONE, excl - edge))
    to_edge = jnp.exp(jnp.where(upper, edge - incl, GONE))
    early_full = split(r * upward, 2)
    late_full = split(k * downward, 2)
    over_full = split(r * past_edge, 2)
    under_full = split(k * to_edge, 2)
    early, over = heads(early_full[0]), heads(over_full[0])
    late, under = late_full[0], under_full[0]
    v2, g2 = heads(vb), heads(gb)
    reached = (r * entering).astype(BF16)
    faded = (k * leaving).astype(BF16)

    s, ga = s_ref[0], ga_ref[0]
    lane_s = lax.broadcasted_iota(jnp.int32, s.shape, 1) < LANE_TOTAL

    def blocks(a):
        return split(
            jnp.concatenate([jnp.where(lane_s, a, 0.0), jnp.where(lane_s, 0.0, a)], axis=0), 2
        )

    (s_diag, s_rest), (g_diag, g_rest) = blocks(s), blocks(ga)

    def both(pieces, axis):
        return jnp.concatenate(pieces, axis=axis)

    scores, inside, across = [], [], []
    for h in range(2):
        scores.append(
            (jnp.where(near, nt(early[h], late), 0.0) + nt(over[h], under)).astype(BF16)
        )
        product = nt(g2[h], vb)
        inside.append(split(jnp.where(near, product, 0.0), 2))
        across.append(split(jnp.where(far, product, 0.0), 2))

    ones = jnp.where(
        (lax.broadcasted_iota(jnp.int32, (PAIR, PAIR), 0) // LANE_TOTAL)
        == (lax.broadcasted_iota(jnp.int32, (PAIR, PAIR), 1) // LANE_TOTAL),
        1.0, 0.0,
    ).astype(BF16)
    present = exact_right(r * u * k, ones, 2)
    agree = exact_right(v * g, ones, 2)

    v_stack, g_stack = both(v2, 0), both(g2, 0)
    mixed = nn(both(scores, 1), v_stack) + nt(reached, s_diag) + present * v
    dv = tn(both(scores, 0), g_stack) + nt(faded, g_diag) + present * g
    def thrice(product, left, right_terms):
        high, rest = (both([product[0][i], product[1][i]], left) for i in range(2))
        main, less = (both(heads(t), 0) for t in right_terms)
        multiply = nn if left == 1 else tn
        return multiply(high, main) + multiply(rest, main) + multiply(high, less)

    memory_r = (
        entering * (nn(gb, s_diag) + nn(gb, s_rest))
        + upward * thrice(inside, 1, late_full)
        + past_edge * thrice(across, 1, under_full)
    )
    memory_k = (
        leaving * (nn(vb, g_diag) + nn(vb, g_rest))
        + downward * thrice(inside, 0, early_full)
        + to_edge * thrice(across, 0, over_full)
    )
    mixed_ref[...] = mixed.astype(BF16)
    dv_ref[...] = dv.astype(BF16)
    dr_ref[...] = (memory_r + u * k * agree).astype(BF16)
    dk_ref[...] = (memory_k + u * r * agree).astype(BF16)
    sums_ref[pl.ds(span + pairs + pair, 1), :] = jnp.sum(r * k * agree, axis=0, keepdims=True)
    coupling = jnp.sum((dec_ref[0] * ga + pull_ref[0]) * s, axis=0, keepdims=True)
    pulled = r * memory_r
    change = k * memory_k - pulled
    fading = coupling + exact_left(triangle(tokens, True), change, 2) - pulled
    slope = fading * w
    sums_ref[pl.ds(span + pair, 1), :] = jnp.sum(slope, axis=0, keepdims=True)
    slope_half = slope.astype(BF16)
    th = th_ref[...]
    db_ref[...] = tn(slope_half, th.astype(BF16))
    back = nn(slope_half, b_ref[...])

    @pl.when(pair == 0)
    def _():
        acc_ref[...] = back

    @pl.when(pair > 0)
    def _():
        acc_ref[...] += back

    @pl.when(pair == pairs - 1)
    def _():
        grad = (acc_ref[...] * (1.0 - th * th)).astype(BF16)

        def part(i, carry):
            c = pl.ds(pl.multiple_of(i * PAIR, PAIR), PAIR)
            dx_ref[:, c] = nt(grad, a_ref[c, :]).astype(BF16)
            sums_ref[c, :] = tn(x_ref[:, c], grad)
            return carry

        lax.fori_loop(0, span // PAIR, part, 0)


def per_device(r, k, v, x, g, a, b, speed, reward):
    r, k, v, x, g = r[0], k[0], v[0], x[0], g[0]
    tokens, span = r.shape
    rank = a.shape[1]
    pairs = span // PAIR
    speed, reward = speed.reshape(pairs, 1, PAIR), reward.reshape(pairs, 1, PAIR)
    whole = lambda shape: pl.BlockSpec(shape, lambda i: (0,) * len(shape))
    cols = pl.BlockSpec((tokens, PAIR), lambda i: (0, i))
    rows = pl.BlockSpec((PAIR, rank), lambda i: (i, 0))
    state = pl.BlockSpec((1, LANE_TOTAL, PAIR), lambda i: (i, 0, 0))
    thin = pl.BlockSpec((1, 1, PAIR), lambda i: (i, 0, 0))
    f32 = lambda *shape: jax.ShapeDtypeStruct(shape, F32)
    b16 = lambda *shape: jax.ShapeDtypeStruct(shape, BF16)
    states = f32(pairs, LANE_TOTAL, PAIR)
    th, w, incl, own, pull, dec = pl.pallas_call(
        totals_kernel,
        grid=(pairs,),
        in_specs=[whole(x.shape), whole(a.shape), rows, thin, cols, cols, cols, cols],
        out_specs=[whole((tokens, rank)), cols, cols, state, state, thin],
        out_shape=[
            f32(tokens, rank), f32(tokens, span), f32(tokens, span), states, states,
            f32(pairs, 1, PAIR),
        ],
        name="totals",
    )(x, a, b, speed, r, k, v, g)
    vmem = pl.BlockSpec(memory_space=pltpu.VMEM)
    dma = pltpu.SemaphoreType.DMA((pairs,))
    s_in, g_after = pl.pallas_call(
        chain_kernel,
        in_specs=[vmem] * 3,
        out_specs=[vmem] * 2,
        out_shape=[states, states],
        scratch_shapes=[
            pltpu.VMEM(states.shape, F32), pltpu.VMEM(states.shape, F32), dma, dma, dma, dma,
        ],
        compiler_params=pltpu.CompilerParams(collective_id=0, has_side_effects=True),
        name="chain",
    )(own, pull, dec)
    height = -(-(span + 2 * pairs) // GRAIN) * GRAIN
    mixed, dr, dk, dv, dx, sums, db = pl.pallas_call(
        finish_kernel,
        grid=(pairs,),
        in_specs=[
            whole(x.shape), whole(a.shape), rows, thin, cols, cols, cols, cols,
            whole((tokens, rank)), cols, cols, state, thin, state, state,
        ],
        out_specs=[
            cols, cols, cols, cols, whole((tokens, span)), whole((height, rank)), rows,
        ],
        out_shape=[
            b16(tokens, span), b16(tokens, span), b16(tokens, span), b16(tokens, span),
            b16(tokens, span), f32(height, rank), f32(span, rank),
        ],
        scratch_shapes=[pltpu.VMEM((tokens, rank), F32)],
        name="finish",
    )(x, a, b, reward, r, k, v, g, th, w, incl, pull, dec, s_in, g_after)

    dp = lax.axis_size("dp")
    place = lax.axis_index("dp")
    first, second = lax.psum((sums, db), ("seq", "dp"))

    def share(array, start, count):
        return lax.dynamic_slice_in_dim(array, start + place * (count // dp), count // dp, 0)

    ga, gb = share(first, 0, span), share(second, 0, span)
    gw = share(first, span, pairs).reshape(span // dp)
    gu = share(first, span + pairs, pairs).reshape(span // dp)
    return (mixed[None], dr[None], dk[None], dv[None], dx[None], ga, gb, gw, gu)


def solution(mesh):
    split_rows = P("dp", "seq", None)
    in_specs = (split_rows,) * 5 + (P(),) * 4
    out_specs = (split_rows,) * 5 + (P("dp", None), P("dp", None), P("dp"), P("dp"))
    return jax.shard_map(
        per_device, mesh=mesh, in_specs=in_specs, out_specs=out_specs, check_vma=False
    )
```
